32 devices in a mesh: seq: 8 (over z, x), head: 4 (over y, core).
Axes of the slice: x: 2, y: 2, z: 4, core: 2. Of those that a mesh axis runs over, the one named last changes fastest.
Arguments:
- hidden: bfloat16 [2048, 4096], P(('seq', 'head')), may hold values from -90 to 90
- block_order: int32 [16], replicated, may hold values from 0 to 15, as said below
- segment_ids: int32 [2048], replicated, may hold values from 0 to 3, never falling along the last dimension, each value on 1 to 1024 neighbouring positions
- w_query: bfloat16 [4096, 4096], P(None, 'head'), may hold values from -0.09375 to 0.09375
- key_weight: bfloat16 [4096, 1024], P(None, 'head'), may hold values from -0.09375 to 0.09375
- value_weight: bfloat16 [4096, 1024], P(None, 'head'), may hold values from -0.09375 to 0.09375
- w_out: bfloat16 [4096, 4096], P('head'), may hold values from -0.09375 to 0.09375
Outputs:
- layer_out: bfloat16 [2048, 4096], P(('seq', 'head'))
The draws below stay inside these ranges and needn't reach their ends.
Inputs may be any that keep to these rules, and one draw needn't show every extreme that they name: `block_order`: for each d, entries 2d and 2d+1 are two block numbers that sum to 15; every block number occurs once.
All inputs are finite; a program needn't handle non-finite values.
Results may differ from the reference program's by a relative error of at most 0.018.
The reference program's roundings to bfloat16 on the way (of `attended`) count: a program that leaves them out, or rounds other values in their place, can miss the bound.
Values may be sent and summed in bfloat16 or wider, within the bound.
A program may use at most 64 MiB of HBM per device.

```python
import math
import jax
import jax.numpy as jnp
import numpy as np
from jax import lax

MODEL_WIDTH = 4096
QUERY_HEADS = 32
KEY_VALUE_HEADS = 8
HEAD_SIZE = 128
TOKENS = 2048
BLK = 128
NBLK = 16
N_HEAD = 4


def draw_hidden(key, part):
    first_key = jax.random.fold_in(key, 0)
    return jnp.clip(jax.random.normal(first_key, (TOKENS, MODEL_WIDTH), jnp.float32), -6.0, 6.0).astype(jnp.bfloat16)


def draw_block_order(key, part):
    first_key, second_key = jax.random.split(jax.random.fold_in(key, 7))
    pairs = NBLK // 2
    shuffled = jax.random.permutation(first_key, pairs).astype(jnp.int32)
    flipped = jax.random.randint(second_key, (pairs,), 0, 2)
    earlier = jnp.where(flipped == 1, shuffled, NBLK - 1 - shuffled)
    later = NBLK - 1 - earlier
    return jnp.stack([earlier, later], axis=1).reshape(NBLK).astype(jnp.int32)


def steps_of(rng, shape, cuts, low, top_value):
    def one(axis_at, shards_of):
        draws = jax.random.uniform(jax.random.fold_in(jax.random.fold_in(rng, 6), axis_at), (shards_of,), jnp.float32, low / len(cuts), top_value / len(cuts))
        return jnp.repeat(jnp.exp(draws), shape[axis_at] // shards_of).reshape((-1,) + (1,) * (len(shape) - axis_at - 1))

    gain = one(*cuts[0])
    for cut in cuts[1:]:
        gain = gain * one(*cut)
    return gain


def length_profile(amount, total, most, slope):
    weights = [(1 << 20) // math.isqrt(rank ** slope) + 1 for rank in range(2, amount + 1)]
    surplus, given = total - most - (amount - 1), [1] * (amount - 1)
    while surplus > 0:
        free = [i for i in range(amount - 1) if given[i] < most]
        pool, left = sum([weights[i] for i in free]), surplus
        for i in free:
            addition = min(most - given[i], max(1, left * weights[i] // pool), surplus)
            given[i] = given[i] + addition
            surplus = surplus - addition
    return np.array([most] + given)


def ragged(own_key, amount, total, limit, slope):
    if amount == 2:
        one = jax.random.randint(own_key, (), max(1, total - limit), min(limit, total - 1) + 1)
        return jnp.stack([one, total - one])
    tallies = jnp.asarray(length_profile(amount, total, limit, slope), jnp.int32)
    pairs = (amount - 1) // 2
    source_of, receiver = tallies[1:1 + 2 * pairs:2], tallies[2:2 + 2 * pairs:2]
    margin = jnp.minimum(source_of - 1, limit - receiver)
    passed = jax.random.randint(jax.random.fold_in(own_key, 1), (pairs,), 0, 1 << 20) % (margin + 1)
    tallies = tallies.at[1:1 + 2 * pairs:2].set(source_of - passed).at[2:2 + 2 * pairs:2].set(receiver + passed)
    return tallies[jax.random.permutation(jax.random.fold_in(own_key, 2), amount)]


def centred(rng, dims, deviation, bound, cuts=(), held_as=jnp.bfloat16):
    values = jax.random.normal(rng, dims, jnp.float32) * deviation
    if len(cuts) > 0:
        values = steps_of(rng, dims, cuts, -0.22, 0.18) * values
    return jnp.clip(values, min=-bound, max=bound).astype(held_as)


def setup_inputs(seed: int = 0) -> dict:
    splits = jax.random.split(jax.random.key(seed), 8)
    hidden = draw_hidden(jax.random.fold_in(splits[7], 71), 0)
    block_order = draw_block_order(jax.random.fold_in(splits[7], 71), 0)
    segment_ids = jnp.searchsorted(jnp.cumsum(ragged(splits[2], 4, TOKENS, TOKENS // 2, 0)), jnp.arange(TOKENS), side="right").astype(jnp.int32)
    w_query = centred(splits[3], (MODEL_WIDTH, QUERY_HEADS * HEAD_SIZE), MODEL_WIDTH ** -0.5, 0.09375, ((1, 4),))
    key_weight = centred(splits[4], (MODEL_WIDTH, KEY_VALUE_HEADS * HEAD_SIZE), MODEL_WIDTH ** -0.5, 0.09375, ((1, 4),))
    value_weight = centred(splits[5], (MODEL_WIDTH, KEY_VALUE_HEADS * HEAD_SIZE), MODEL_WIDTH ** -0.5, 0.09375, ((1, 4),))
    w_out = centred(splits[6], (QUERY_HEADS * HEAD_SIZE, MODEL_WIDTH), (QUERY_HEADS * HEAD_SIZE) ** -0.5, 0.09375, ((0, 4),))
    return {"hidden": hidden, "block_order": block_order, "segment_ids": segment_ids, "w_query": w_query, "key_weight": key_weight, "value_weight": value_weight, "w_out": w_out}


NEGATIVE_FILLER = -1e30
ROPE_BASE = 500000.0


def apply_rotary(values, block_places, heads):
    count_rows = values.shape[0]
    shaped = values.reshape(count_rows, heads, HEAD_SIZE)
    half_dim = HEAD_SIZE // 2
    freqs = ROPE_BASE ** (-(jnp.arange(half_dim, dtype=jnp.float32) * 2.0 / HEAD_SIZE))
    angles = block_places.astype(jnp.float32)[:, None] * freqs[None, :]
    cosine = jnp.cos(angles)[:, None, :]
    sine = jnp.sin(angles)[:, None, :]
    first_half = shaped[:, :, :half_dim]
    second_half = shaped[:, :, half_dim:]
    turned = jnp.concatenate([first_half * cosine - second_half * sine, second_half * cosine + first_half * sine], axis=2)
    return turned.reshape(count_rows, heads * HEAD_SIZE)


def attend(carry_state, query_matrix, query_pos, query_seg, key_block, value_block, key_pos, key_seg):
    running, totals, weighted = carry_state
    scores = jnp.einsum("qhgd,khd->hgqk", query_matrix.astype(jnp.float32), key_block.astype(jnp.float32)) * (HEAD_SIZE ** -0.5)
    allowed = (key_pos[None, :] <= query_pos[:, None]) & (key_seg[None, :] == query_seg[:, None])
    masked = jnp.where(allowed, scores, NEGATIVE_FILLER)
    newmax = jnp.maximum(running, jnp.max(masked, axis=3))
    expo = jnp.where(allowed, jnp.exp(scores - newmax[..., None]), 0.0)
    factor = jnp.exp(running - newmax)
    totals = totals * factor + jnp.sum(expo, axis=3)
    rounded = expo.astype(jnp.bfloat16).astype(jnp.float32)
    weighted = weighted * factor[..., None] + jnp.einsum("hgqk,khd->hgqd", rounded, value_block.astype(jnp.float32))
    return newmax, totals, weighted


def reference(hidden, block_order, segment_ids, w_query, key_weight, value_weight, w_out):
    inverse = jnp.zeros((NBLK,), jnp.int32).at[block_order].set(jnp.arange(NBLK, dtype=jnp.int32))
    sorted_blocks = hidden.reshape(NBLK, BLK, MODEL_WIDTH)[inverse].reshape(TOKENS, MODEL_WIDTH)
    block_places = jnp.arange(TOKENS, dtype=jnp.int32)
    query_matrix = apply_rotary(jnp.dot(sorted_blocks, w_query, preferred_element_type=jnp.float32), block_places, QUERY_HEADS).astype(jnp.bfloat16)
    every_key = apply_rotary(jnp.dot(sorted_blocks, key_weight, preferred_element_type=jnp.float32), block_places, KEY_VALUE_HEADS).astype(jnp.bfloat16)
    every_value = jnp.dot(sorted_blocks, value_weight, preferred_element_type=jnp.float32).astype(jnp.bfloat16)
    query_group = QUERY_HEADS // KEY_VALUE_HEADS
    query_block = math.gcd(512, TOKENS)
    nblocks = TOKENS // query_block

    def outer(index, outputs):
        starting_row = (index * query_block).astype(jnp.int32)
        query_rows = lax.dynamic_slice_in_dim(query_matrix, starting_row, query_block, 0).reshape(query_block, KEY_VALUE_HEADS, query_group, HEAD_SIZE)
        qpos = starting_row + jnp.arange(query_block, dtype=jnp.int32)
        qseg = lax.dynamic_slice_in_dim(segment_ids, starting_row, query_block, 0)
        start_state = (jnp.full((KEY_VALUE_HEADS, query_group, query_block), NEGATIVE_FILLER, jnp.float32),
                   jnp.zeros((KEY_VALUE_HEADS, query_group, query_block), jnp.float32),
                   jnp.zeros((KEY_VALUE_HEADS, query_group, query_block, HEAD_SIZE), jnp.float32))

        def inner_loop(key_index, carry_state):
            leading_key = (key_index * query_block).astype(jnp.int32)
            key_block = lax.dynamic_slice_in_dim(every_key, leading_key, query_block, 0).reshape(query_block, KEY_VALUE_HEADS, HEAD_SIZE)
            value_block = lax.dynamic_slice_in_dim(every_value, leading_key, query_block, 0).reshape(query_block, KEY_VALUE_HEADS, HEAD_SIZE)
            key_pos = leading_key + jnp.arange(query_block, dtype=jnp.int32)
            key_seg = lax.dynamic_slice_in_dim(segment_ids, leading_key, query_block, 0)
            return attend(carry_state, query_rows, qpos, qseg, key_block, value_block, key_pos, key_seg)

        finished = lax.fori_loop(0, index + 1, inner_loop, start_state)
        block_out = (finished[2] / finished[1][..., None]).transpose(2, 0, 1, 3).reshape(query_block, QUERY_HEADS * HEAD_SIZE)
        return lax.dynamic_update_slice_in_dim(outputs, block_out.astype(jnp.bfloat16), starting_row, 0)

    attended = lax.fori_loop(0, nblocks, outer, jnp.zeros((TOKENS, QUERY_HEADS * HEAD_SIZE), jnp.bfloat16))
    width = QUERY_HEADS * HEAD_SIZE // N_HEAD
    summed = jnp.zeros((TOKENS, MODEL_WIDTH), jnp.float32)
    for member in range(N_HEAD):
        partial_sum = jnp.dot(attended[:, member * width:(member + 1) * width], w_out[member * width:(member + 1) * width], preferred_element_type=jnp.float32)
        summed = summed + partial_sum.astype(jnp.bfloat16).astype(jnp.float32)
    result = summed.astype(jnp.bfloat16).reshape(NBLK, BLK, MODEL_WIDTH)[block_order].reshape(TOKENS, MODEL_WIDTH)
    return result
```

```python
import functools
import math

import jax
import jax.numpy as jnp
import numpy as np
from jax import lax
from jax.experimental import pallas as pl
from jax.experimental.pallas import tpu as pltpu
from jax.sharding import PartitionSpec as P

HEAD_SIZE = 128
NEGATIVE_FILLER = -1e30
ROPE_BASE = 500000.0
DOCS = 4
CORES = 2
MESH = pl.DeviceIdType.MESH
F32 = jnp.float32
BF16 = jnp.bfloat16


def rotated(t, cosine, sine):
    heads = t.shape[1] // HEAD_SIZE
    pieces = []
    for h in range(heads):
        one = t[:, h * HEAD_SIZE:(h + 1) * HEAD_SIZE]
        pieces.append(one * cosine + pltpu.roll(one, HEAD_SIZE // 2, 1) * sine)
    return pieces


def kernel(
    X, Z, Y, NC, NO,
    order, hidden, seg, freq, wq, wk, wv, wo_hbm, out,
    xg, wb, wo, acc, cos_t, sin_t, q, kv, bias, m_s, l_s, o_s, att, pb, rb, sb, fb, info,
    w_sem, wo_sem, hs_sem, hp_sem, hl_sem, hr_sem, ks_sem, kr_sem, ps_sem, pr_sem, ys_sem, yr_sem,
):
    r, D = hidden.shape
    R = xg.shape[0]
    G = R // Y
    Cq, Ck = wq.shape[1], wk.shape[1]
    half = R // 2
    q_heads, kv_heads = Cq // HEAD_SIZE, Ck // HEAD_SIZE
    group = q_heads // kv_heads
    KW, NW = D // NC, D // NO
    s_id, h_id = lax.axis_index("seq"), lax.axis_index("head")
    y, c = h_id // CORES, h_id % CORES
    z, x = s_id // X, s_id % X
    partner = y * CORES + (1 - c)

    def peer_y(j):
        return lax.rem(y + j, Y)

    def w_copy(which, k):
        src = (wq, wk, wv)[which]
        col = (0, Cq, Cq + Ck)[which]
        rows = pl.ds(k * KW, KW)
        return pltpu.make_async_copy(
            src.at[rows, :], wb.at[rows, pl.ds(col, src.shape[1])], w_sem.at[which, k]
        )

    def wo_copy(n):
        cols = pl.ds(n * NW, NW)
        return pltpu.make_async_copy(wo_hbm.at[:, cols], wo.at[:, cols], wo_sem.at[n])

    for k in range(NC):
        w_copy(1, k).start()
        w_copy(2, k).start()
    for k in range(NC):
        w_copy(0, k).start()

    barrier = pltpu.get_barrier_semaphore()

    def greet(sq, hd):
        pl.semaphore_signal(barrier, inc=1, device_id=(sq, hd), device_id_type=MESH)

    greet(s_id, partner)
    for j in range(1, Y):
        greet(s_id, peer_y(j) * CORES + c)
    for k in range(1, X):
        greet(z * X + lax.rem(x + k, X), h_id)

    @pl.when(z > 0)
    def _():
        greet(s_id - X, h_id)

    @pl.when(z < Z - 1)
    def _():
        greet(s_id + X, h_id)

    near = jnp.where(z > 0, 1, 0) + jnp.where(z < Z - 1, 1, 0)
    pl.semaphore_wait(barrier, 1 + (Y - 1) + (X - 1) + near)

    def hid_copy(origin, k, target, sem, from_input):
        cols = pl.ds(k * KW, KW)
        rows = pl.ds(origin * r, r)
        src = hidden.at[:, cols] if from_input else xg.at[rows, cols]
        return pltpu.make_async_remote_copy(
            src_ref=src, dst_ref=xg.at[rows, cols], send_sem=sem, recv_sem=hr_sem.at[origin, k],
            device_id=(s_id, target), device_id_type=MESH,
        )

    def hid_send(j, k):
        return hid_copy(h_id, k, peer_y(j) * CORES + c, hs_sem.at[j, k], True)

    def hid_pair(k):
        return hid_copy(h_id, k, partner, hp_sem.at[k], True)

    def hid_relay(j, k):
        return hid_copy(peer_y(j) * CORES + c, k, partner, hl_sem.at[j, k], False)

    def hid_from(origin, k):
        return hid_copy(origin, k, partner, hp_sem.at[k], False)

    for k in range(NC):
        hid_pair(k).start()
        for j in range(1, Y):
            hid_send(j, k).start()
    for n in range(NO):
        wo_copy(n).start()

    xg[pl.ds(h_id * r, r), :] = hidden[...]

    lane = lax.broadcasted_iota(jnp.int32, (half, HEAD_SIZE), 1)
    row = lax.broadcasted_iota(jnp.int32, (half, HEAD_SIZE), 0)
    for i in range(2):
        base = order[2 * s_id + i]
        angle = (row + base * half).astype(F32) * freq[...]
        cos_t[pl.ds(i * half, half), :] = jnp.cos(angle)
        sn = jnp.sin(angle)
        sin_t[pl.ds(i * half, half), :] = jnp.where(lane < HEAD_SIZE // 2, -sn, sn)
        brow = lax.broadcasted_iota(jnp.int32, seg.shape, 0)
        mine = jnp.sum(jnp.where(brow == base, seg[...], 0), axis=0, keepdims=True)
        start = jnp.zeros_like(mine)
        for v in range(1, DOCS):
            below = jnp.sum(
                jnp.sum((seg[...] < v).astype(jnp.int32), axis=0, keepdims=True), axis=1, keepdims=True
            )
            start = jnp.where(mine == v, below, start)
        info[0:1, i * half:(i + 1) * half] = (
            lax.broadcasted_iota(jnp.int32, (1, half), 1) + base * half
        )
        info[1:2, i * half:(i + 1) * half] = start

    def kv_copy(zb, xb, g, target, way):
        slot = zb * X + xb
        rows = pl.ds(g * G, G)
        return pltpu.make_async_remote_copy(
            src_ref=kv.at[slot, rows, :], dst_ref=kv.at[slot, rows, :],
            send_sem=ks_sem.at[zb, g, way], recv_sem=kr_sem.at[slot, g],
            device_id=(target, h_id), device_id_type=MESH,
        )

    def kv_out(zb, g, up, down, act):
        @pl.when(up & (z < Z - 1))
        def _():
            act(kv_copy(zb, x, g, s_id + X, 0))

        @pl.when(down & (z > 0))
        def _():
            act(kv_copy(zb, x, g, s_id - X, 1))

        for k in range(1, X):
            act(kv_copy(zb, x, g, z * X + lax.rem(x + k, X), 1 + k))

    def kv_wait(zb, xb, g):
        kv_copy(zb, xb, g, s_id, 0).wait_recv()

    start_it = lambda cp: cp.start()
    sent = lambda cp: cp.wait_send()

    def forward(d, g):
        @pl.when((d < Z) & (z - d >= 0))
        def _():
            kv_wait(z - d, x, g)
            kv_out(z - d, g, True, False, start_it)

        @pl.when((d < Z) & (z + d < Z))
        def _():
            kv_wait(z + d, x, g)
            kv_out(z + d, g, False, True, start_it)

    def store_kv(g):
        rows = pl.ds(g * G, G)
        pieces = rotated(acc[:, Cq:Cq + Ck], cos_t[rows, :], sin_t[rows, :])
        for h in range(kv_heads):
            kv[s_id, rows, h * HEAD_SIZE:(h + 1) * HEAD_SIZE] = pieces[h].astype(BF16)
        kv[s_id, rows, Ck:2 * Ck] = acc[:, Cq + Ck:].astype(BF16)
        kv_out(z, g, True, True, start_it)

    def store_q(g):
        rows = pl.ds(g * G, G)
        pieces = rotated(acc[:, :Cq], cos_t[rows, :], sin_t[rows, :])
        for h in range(q_heads):
            q[rows, h * HEAD_SIZE:(h + 1) * HEAD_SIZE] = pieces[h].astype(BF16)

    def add_dot(g, k, lo, hi):
        span = pl.ds(k * KW, KW)
        acc[:, lo:hi] += jnp.dot(
            xg[pl.ds(g * G, G), span], wb[span, lo:hi], preferred_element_type=F32
        )

    acc[...] = jnp.zeros_like(acc)

    def first_kv(k, _):
        hid_from(partner, k).wait_recv()
        w_copy(1, k).wait()
        w_copy(2, k).wait()
        add_dot(y, k, Cq, Cq + 2 * Ck)
        return 0

    lax.fori_loop(0, NC, first_kv, 0)
    store_kv(y)

    def first_q(k, _):
        w_copy(0, k).wait()
        add_dot(y, k, 0, Cq)
        return 0

    lax.fori_loop(0, NC, first_q, 0)
    store_q(y)

    for j in range(1, Y):
        g = peer_y(j)
        acc[...] = jnp.zeros_like(acc)

        def arrive(k, _, j=j, g=g):
            @pl.when(k < NC)
            def _():
                hid_from(g * CORES + c, k).wait_recv()
                hid_relay(j, k).start()

            @pl.when(k > 0)
            def _():
                hid_from(g * CORES + (1 - c), k - 1).wait_recv()
                add_dot(g, k - 1, 0, Cq + 2 * Ck)

            if j == 1:
                @pl.when(k == NC // 2)
                def _():
                    forward(1, y)

            return 0

        lax.fori_loop(0, NC + 1, arrive, 0)
        store_kv(g)
        store_q(g)

    m_s[...] = jnp.full_like(m_s, NEGATIVE_FILLER)
    l_s[...] = jnp.zeros_like(l_s)
    o_s[...] = jnp.zeros_like(o_s)
    scale = math.log2(math.e) / math.sqrt(HEAD_SIZE)
    nt = (((1,), (1,)), ((), ()))

    def attend(slot):
        krow = lax.broadcasted_iota(jnp.int32, (half, R), 0)
        for i in range(2):
            kpos = krow + order[2 * slot + i] * half
            ok = (kpos <= info[0:1, :]) & (kpos >= info[1:2, :])
            bias[i * half:(i + 1) * half, :] = jnp.where(ok, 0.0, NEGATIVE_FILLER)
        for kh in range(kv_heads):
            keys = kv[slot, :, kh * HEAD_SIZE:(kh + 1) * HEAD_SIZE]
            vals = kv[slot, :, Ck + kh * HEAD_SIZE:Ck + (kh + 1) * HEAD_SIZE].T
            for gh in range(group):
                h = kh * group + gh
                cols = slice(h * HEAD_SIZE, (h + 1) * HEAD_SIZE)
                s = lax.dot_general(keys, q[:, cols], nt, preferred_element_type=F32)
                s = s * scale + bias[...]
                old = m_s[h:h + 1, :]
                new = jnp.maximum(old, jnp.max(s, axis=0, keepdims=True))
                p = jnp.exp2(s - new)
                alpha = jnp.exp2(old - new)
                m_s[h:h + 1, :] = new
                l_s[h:h + 1, :] = l_s[h:h + 1, :] * alpha + jnp.sum(p, axis=0, keepdims=True)
                o_s[cols, :] = o_s[cols, :] * alpha + jnp.dot(
                    vals, p.astype(BF16), preferred_element_type=F32
                )

    def stage(d, _):
        @pl.when(d >= 1)
        def _():
            for j in range(1, Y):
                forward(d, peer_y(j))
            forward(d + 1, y)

        def visit(i, _):
            side, k = i // X, lax.rem(i, X)
            dist = jnp.where(k == 0, d, d - 1)
            zb = jnp.where(side == 0, z - dist, z + dist)
            xb = lax.rem(x + k, X)
            ok = (zb >= 0) & (zb < Z) & (dist >= 0) & ((dist > 0) | (side == 0))

            @pl.when(ok)
            def _():
                @pl.when(k > 0)
                def _():
                    for g in range(Y):
                        kv_wait(zb, xb, g)

                attend(zb * X + xb)

            return 0

        lax.fori_loop(0, 2 * X, visit, 0)
        return 0

    lax.fori_loop(0, Z + 1, stage, 0)

    for h in range(q_heads):
        cols = slice(h * HEAD_SIZE, (h + 1) * HEAD_SIZE)
        att[:, cols] = (o_s[cols, :] / l_s[h:h + 1, :]).T.astype(BF16)

    def pair_copy(j, n):
        cols = pl.ds(n * NW, NW)
        return pltpu.make_async_remote_copy(
            src_ref=pb.at[j, 1 - c, :, cols], dst_ref=rb.at[j, :, cols],
            send_sem=ps_sem.at[j, n], recv_sem=pr_sem.at[j, n],
            device_id=(s_id, partner), device_id_type=MESH,
        )

    def far_copy(j, n):
        cols = pl.ds(n * NW, NW)
        return pltpu.make_async_remote_copy(
            src_ref=sb.at[j, :, cols], dst_ref=fb.at[j, :, cols],
            send_sem=ys_sem.at[j, n], recv_sem=yr_sem.at[j, n],
            device_id=(s_id, peer_y(j + 1) * CORES + c), device_id_type=MESH,
        )

    def pair_sum(j, n):
        cols = pl.ds(n * NW, NW)
        pair_copy(j, n).wait_recv()
        return pb[j, c, :, cols].astype(F32) + rb[j, :, cols].astype(F32)

    def project(i, _):
        @pl.when(i < Y * NO)
        def _():
            j, n = i // NO, lax.rem(i, NO)
            cols = pl.ds(n * NW, NW)

            @pl.when(j == 0)
            def _():
                wo_copy(n).wait()

            part = jnp.dot(
                att[pl.ds(peer_y(j + 1) * G, G), :], wo[:, cols], preferred_element_type=F32
            ).astype(BF16)
            for e in range(CORES):
                pb[j, e, :, cols] = part[e * r:(e + 1) * r, :]
            pair_copy(j, n).start()

        @pl.when((i > 0) & (i <= (Y - 1) * NO))
        def _():
            j, n = (i - 1) // NO, lax.rem(i - 1, NO)
            sb[j, :, pl.ds(n * NW, NW)] = pair_sum(j, n).astype(BF16)
            far_copy(j, n).start()

        return 0

    lax.fori_loop(0, Y * NO, project, 0)

    def finish(n, _):
        total = pair_sum(Y - 1, n)
        for j in range(Y - 1):
            far_copy(j, n).wait_recv()
            total = total + fb[j, :, pl.ds(n * NW, NW)].astype(F32)
        out[:, pl.ds(n * NW, NW)] = total.astype(BF16)
        return 0

    lax.fori_loop(0, NO, finish, 0)

    def drain_hidden(k, _):
        hid_pair(k).wait_send()
        for j in range(1, Y):
            hid_send(j, k).wait_send()
            hid_relay(j, k).wait_send()
        return 0

    lax.fori_loop(0, NC, drain_hidden, 0)

    def drain_kv(zb, _):
        for g in range(Y):
            kv_out(zb, g, zb <= z, zb >= z, sent)
        return 0

    lax.fori_loop(0, Z, drain_kv, 0)

    def drain_out(n, _):
        for j in range(Y):
            pair_copy(j, n).wait_send()
        for j in range(Y - 1):
            far_copy(j, n).wait_send()
        return 0

    lax.fori_loop(0, NO, drain_out, 0)


def on_device(X, Z, Y, hidden, block_order, segment_ids, w_query, key_weight, value_weight, w_out):
    r, D = hidden.shape
    S, H = X * Z, Y * CORES
    R = r * H
    G = R // Y
    Cq, Ck = w_query.shape[1], key_weight.shape[1]
    W = Cq + 2 * Ck
    q_heads = Cq // HEAD_SIZE
    NC = NO = max(1, D // 512)
    exponent = np.arange(HEAD_SIZE // 2, dtype=np.float64) * 2.0 / HEAD_SIZE
    freqs = np.tile(ROPE_BASE ** (-exponent), 2).astype(np.float32)[None, :]
    dma = pltpu.SemaphoreType.DMA
    far = max(1, Y - 1)
    vmem = pl.BlockSpec(memory_space=pltpu.VMEM)
    anywhere = pl.BlockSpec(memory_space=pl.ANY)
    return pl.pallas_call(
        functools.partial(kernel, X, Z, Y, NC, NO),
        out_shape=jax.ShapeDtypeStruct((r, D), BF16),
        in_specs=[pl.BlockSpec(memory_space=pltpu.SMEM), vmem, vmem, vmem] + [anywhere] * 4,
        out_specs=vmem,
        scratch_shapes=[
            pltpu.VMEM((R, D), BF16),
            pltpu.VMEM((D, W), BF16),
            pltpu.VMEM((Cq, D), BF16),
            pltpu.VMEM((G, W), F32),
            pltpu.VMEM((R, HEAD_SIZE), F32),
            pltpu.VMEM((R, HEAD_SIZE), F32),
            pltpu.VMEM((R, Cq), BF16),
            pltpu.VMEM((S, R, 2 * Ck), BF16),
            pltpu.VMEM((R, R), F32),
            pltpu.VMEM((q_heads, R), F32),
            pltpu.VMEM((q_heads, R), F32),
            pltpu.VMEM((Cq, R), F32),
            pltpu.VMEM((R, Cq), BF16),
            pltpu.VMEM((Y, CORES, r, D), BF16),
            pltpu.VMEM((Y, r, D), BF16),
            pltpu.VMEM((far, r, D), BF16),
            pltpu.VMEM((far, r, D), BF16),
            pltpu.VMEM((2, R), jnp.int32),
            dma((3, NC)), dma((NO,)),
            dma((Y, NC)), dma((NC,)), dma((Y, NC)), dma((H, NC)),
            dma((Z, Y, 1 + X)), dma((S, Y)),
            dma((Y, NO)), dma((Y, NO)), dma((far, NO)), dma((far, NO)),
        ],
        compiler_params=pltpu.CompilerParams(
            collective_id=0, has_side_effects=True, vmem_limit_bytes=60 * 1024 * 1024
        ),
    )(
        block_order, hidden, segment_ids.reshape(block_order.shape[0], -1), jnp.asarray(freqs),
        w_query, key_weight, value_weight, w_out,
    )


def solution(mesh):
    seq, head = mesh.shape["seq"], mesh.shape["head"]
    X = 1
    while 4 * X * X <= seq and seq % (2 * X) == 0:
        X *= 2
    placed = (
        P(("seq", "head"), None),
        P(),
        P(),
        P(None, "head"),
        P(None, "head"),
        P(None, "head"),
        P("head", None),
    )
    return jax.shard_map(
        functools.partial(on_device, X, seq // X, head // CORES),
        mesh=mesh, in_specs=placed, out_specs=P(("seq", "head"), None), check_vma=False,
    )
```

```python
import functools
import math

import jax
import jax.numpy as jnp
import numpy as np
from jax import lax
from jax.experimental import pallas as pl
from jax.experimental.pallas import tpu as pltpu
from jax.sharding import PartitionSpec as P

HEAD_SIZE = 128
NEGATIVE_FILLER = -1e30
ROPE_BASE = 500000.0
DOCS = 4
CORES = 2
SUB = 2
EARLY = 1
MESH = pl.DeviceIdType.MESH
F32 = jnp.float32
BF16 = jnp.bfloat16


def rotated(t, cosine, sine):
    heads = t.shape[1] // HEAD_SIZE
    pieces = []
    for h in range(heads):
        one = t[:, h * HEAD_SIZE:(h + 1) * HEAD_SIZE]
        pieces.append(one * cosine + pltpu.roll(one, HEAD_SIZE // 2, 1) * sine)
    return pieces


def kernel(
    X, Z, Y, NC, NO,
    order, hidden, seg, freq, wq, wk, wv, wo_hbm, out,
    xg, wb, wo, acc, cos_t, sin_t, kv, att, pb, rb, sb, fb, *rest,
):
    far_side, near_side = rest[:6], rest[6:12]
    (w_sem, wo_sem, hs_sem, hp_sem, hl_sem, hr_sem,
     ks_sem, kr_sem, ps_sem, pr_sem, ys_sem, yr_sem) = rest[12:]
    r, D = hidden.shape
    R = xg.shape[0]
    G = R // Y
    Cq, Ck = wq.shape[1], wk.shape[1]
    half = R // 2
    q_heads, kv_heads = Cq // HEAD_SIZE, Ck // HEAD_SIZE
    group = q_heads // kv_heads
    KW, NW = D // NC, D // NO
    s_id, h_id = lax.axis_index("seq"), lax.axis_index("head")
    y, c = h_id // CORES, h_id % CORES
    z, x = s_id // X, s_id % X
    partner = y * CORES + (1 - c)

    def peer_y(j):
        return lax.rem(y + j, Y)

    def w_copy(which, k):
        src = (wq, wk, wv)[which]
        col = (0, Cq, Cq + Ck)[which]
        rows = pl.ds(k * KW, KW)
        return pltpu.make_async_copy(
            src.at[rows, :], wb.at[rows, pl.ds(col, src.shape[1])], w_sem.at[which, k]
        )

    def wo_copy(n):
        cols = pl.ds(n * NW, NW)
        return pltpu.make_async_copy(wo_hbm.at[:, cols], wo.at[:, cols], wo_sem.at[n])

    for k in range(NC):
        w_copy(1, k).start()
        w_copy(2, k).start()
    for k in range(NC):
        w_copy(0, k).start()

    barrier = pltpu.get_barrier_semaphore()

    def greet(sq, hd):
        pl.semaphore_signal(barrier, inc=1, device_id=(sq, hd), device_id_type=MESH)

    greet(s_id, partner)
    for j in range(1, Y):
        greet(s_id, peer_y(j) * CORES + c)
    for k in range(1, X):
        greet(z * X + lax.rem(x + k, X), h_id)

    @pl.when(z > 0)
    def _():
        greet(s_id - X, h_id)

    @pl.when(z < Z - 1)
    def _():
        greet(s_id + X, h_id)

    near = jnp.where(z > 0, 1, 0) + jnp.where(z < Z - 1, 1, 0)
    pl.semaphore_wait(barrier, 1 + (Y - 1) + (X - 1) + near)

    def hid_copy(origin, k, target, sem, from_input):
        cols = pl.ds(k * KW, KW)
        rows = pl.ds(origin * r, r)
        src = hidden.at[:, cols] if from_input else xg.at[rows, cols]
        return pltpu.make_async_remote_copy(
            src_ref=src, dst_ref=xg.at[rows, cols], send_sem=sem, recv_sem=hr_sem.at[origin, k],
            device_id=(s_id, target), device_id_type=MESH,
        )

    def hid_send(j, k):
        return hid_copy(h_id, k, peer_y(j) * CORES + c, hs_sem.at[j, k], True)

    def hid_pair(k):
        return hid_copy(h_id, k, partner, hp_sem.at[k], True)

    def hid_relay(j, k):
        return hid_copy(peer_y(j) * CORES + c, k, partner, hl_sem.at[j, k], False)

    def hid_from(origin, k):
        return hid_copy(origin, k, partner, hp_sem.at[k], False)

    for k in range(NC):
        hid_pair(k).start()
        for j in range(1, Y):
            hid_send(j, k).start()
    for n in range(NO):
        wo_copy(n).start()

    xg[pl.ds(h_id * r, r), :] = hidden[...]

    lane = lax.broadcasted_iota(jnp.int32, (half, HEAD_SIZE), 1)
    row = lax.broadcasted_iota(jnp.int32, (half, HEAD_SIZE), 0)
    for i in range(2):
        base = order[2 * s_id + i]
        angle = (row + base * half).astype(F32) * freq[...]
        cos_t[pl.ds(i * half, half), :] = jnp.cos(angle)
        sn = jnp.sin(angle)
        sin_t[pl.ds(i * half, half), :] = jnp.where(lane < HEAD_SIZE // 2, -sn, sn)

    starts = [
        jnp.sum(jnp.sum((seg[...] < v).astype(jnp.int32), axis=0, keepdims=True), axis=1, keepdims=True)
        for v in range(1, DOCS)
    ]
    for side, places in ((far_side, range(1, Y)), (near_side, (0,))):
        info = side[5]
        for i, j in enumerate(places):
            first = peer_y(j) * G
            pos = lax.broadcasted_iota(jnp.int32, (1, G), 1) + (
                order[2 * s_id + first // half] * half + lax.rem(first, half)
            )
            start = jnp.zeros_like(pos)
            for begun in starts:
                start = jnp.where(begun <= pos, jnp.maximum(start, begun), start)
            wide = len(places) * G
            for gh in range(info.shape[1] // wide):
                lanes = slice(gh * wide + i * G, gh * wide + (i + 1) * G)
                info[0:1, lanes] = pos
                info[1:2, lanes] = start

    B = G // SUB

    def kv_copy(zb, xb, u, target, way):
        slot = zb * X + xb
        rows = pl.ds(u * B, B)
        return pltpu.make_async_remote_copy(
            src_ref=kv.at[slot, rows, :], dst_ref=kv.at[slot, rows, :],
            send_sem=ks_sem.at[zb, u, way], recv_sem=kr_sem.at[slot, u],
            device_id=(target, h_id), device_id_type=MESH,
        )

    def kv_out(zb, u, up, down, act):
        @pl.when(up & (z < Z - 1))
        def _():
            act(kv_copy(zb, x, u, s_id + X, 0))

        @pl.when(down & (z > 0))
        def _():
            act(kv_copy(zb, x, u, s_id - X, 1))

        for k in range(1, X):
            act(kv_copy(zb, x, u, z * X + lax.rem(x + k, X), 1 + k))

    def kv_wait(zb, xb, u):
        kv_copy(zb, xb, u, s_id, 0).wait_recv()

    start_it = lambda cp: cp.start()
    sent = lambda cp: cp.wait_send()

    def forward(d, g):
        for e in range(SUB):
            u = g * SUB + e

            @pl.when((d < Z) & (z - d >= 0))
            def _():
                kv_wait(z - d, x, u)
                kv_out(z - d, u, True, False, start_it)

            @pl.when((d < Z) & (z + d < Z))
            def _():
                kv_wait(z + d, x, u)
                kv_out(z + d, u, False, True, start_it)

    def store_kv(g):
        rows = pl.ds(g * G, G)
        pieces = rotated(acc[:, Cq:Cq + Ck], cos_t[rows, :], sin_t[rows, :])
        for h in range(kv_heads):
            kv[s_id, rows, h * HEAD_SIZE:(h + 1) * HEAD_SIZE] = pieces[h].astype(BF16)
        kv[s_id, rows, Ck:2 * Ck] = acc[:, Cq + Ck:].astype(BF16)
        for e in range(SUB):
            kv_out(z, g * SUB + e, True, True, start_it)

    def store_q(g, side, place):
        rows = pl.ds(g * G, G)
        q = side[0]
        wide = q.shape[1] // group
        pieces = rotated(acc[:, :Cq], cos_t[rows, :], sin_t[rows, :])
        for h in range(q_heads):
            lo = (h % group) * wide + place * G
            q[h // group, lo:lo + G, :] = pieces[h].astype(BF16)

    def add_dot(g, k, lo, hi):
        span = pl.ds(k * KW, KW)
        acc[:, lo:hi] += jnp.dot(
            xg[pl.ds(g * G, G), span], wb[span, lo:hi], preferred_element_type=F32
        )

    acc[...] = jnp.zeros_like(acc)

    def first_kv(k, _):
        hid_from(partner, k).wait_recv()
        w_copy(1, k).wait()
        w_copy(2, k).wait()
        add_dot(y, k, Cq, Cq + 2 * Ck)
        return 0

    lax.fori_loop(0, NC, first_kv, 0)
    store_kv(y)

    def first_q(k, _):
        w_copy(0, k).wait()
        add_dot(y, k, 0, Cq)
        return 0

    lax.fori_loop(0, NC, first_q, 0)
    store_q(y, near_side, 0)

    for j in range(1, Y):
        g = peer_y(j)
        acc[...] = jnp.zeros_like(acc)

        def arrive(k, _, j=j, g=g):
            @pl.when(k < NC)
            def _():
                hid_from(g * CORES + c, k).wait_recv()
                hid_relay(j, k).start()

            @pl.when(k > 0)
            def _():
                hid_from(g * CORES + (1 - c), k - 1).wait_recv()
                add_dot(g, k - 1, 0, Cq + 2 * Ck)

            if j == 1:
                @pl.when(k == NC // 2)
                def _():
                    forward(1, y)

                @pl.when(k == NC)
                def _():
                    forward(2, y)

            return 0

        lax.fori_loop(0, NC + 1, arrive, 0)
        store_kv(g)
        store_q(g, far_side, j - 1)

    for side in (far_side, near_side):
        side[1][...] = jnp.full_like(side[1], NEGATIVE_FILLER)
        side[2][...] = jnp.zeros_like(side[2])
        side[3][...] = jnp.zeros_like(side[3])
    scale = math.log2(math.e) / math.sqrt(HEAD_SIZE)
    nt = (((1,), (1,)), ((), ()))

    def attend(slot, side):
        q, m_s, l_s, o_s, bias, info = side
        chunk = bias.shape[1]
        krow = lax.broadcasted_iota(jnp.int32, (half, chunk), 0)
        for i in range(2):
            kpos = krow + order[2 * slot + i] * half
            ok = (kpos <= info[0:1, :]) & (kpos >= info[1:2, :])
            bias[i * half:(i + 1) * half, :] = jnp.where(ok, 0.0, NEGATIVE_FILLER)
        work = [(kh, w) for kh in range(kv_heads) for w in range(q.shape[1] // chunk)]
        span = lambda w: slice(w * chunk, (w + 1) * chunk)
        keys = [kv[slot, :, kh * HEAD_SIZE:(kh + 1) * HEAD_SIZE] for kh in range(kv_heads)]
        vals = [
            kv[slot, :, Ck + kh * HEAD_SIZE:Ck + (kh + 1) * HEAD_SIZE].T for kh in range(kv_heads)
        ]

        def scores(item):
            kh, w = item
            return lax.dot_general(keys[kh], q[kh, span(w), :], nt, preferred_element_type=F32)

        ahead = scores(work[0])
        for i, (kh, w) in enumerate(work):
            raw = ahead
            if i + 1 < len(work):
                ahead = scores(work[i + 1])
            cols = span(w)
            s = raw * scale + bias[...]
            old = m_s[kh:kh + 1, cols]
            new = jnp.maximum(old, jnp.max(s, axis=0, keepdims=True))
            p = jnp.exp2(s - new)
            alpha = jnp.exp2(old - new)
            m_s[kh:kh + 1, cols] = new
            l_s[kh:kh + 1, cols] = l_s[kh:kh + 1, cols] * alpha + jnp.sum(p, axis=0, keepdims=True)
            o_s[kh, :, cols] = o_s[kh, :, cols] * alpha + jnp.dot(
                vals[kh], p.astype(BF16), preferred_element_type=F32
            )

    def settle(side, lo):
        q, m_s, l_s, o_s, bias, info = side
        wide = q.shape[1] // group
        for h in range(q_heads):
            kh, gh = h // group, h % group
            lanes = slice(gh * wide, (gh + 1) * wide)
            att[lo:lo + wide, h * HEAD_SIZE:(h + 1) * HEAD_SIZE] = (
                o_s[kh, :, lanes] / l_s[kh:kh + 1, lanes]
            ).T.astype(BF16)

    def early(dist, xb):
        return (xb == x) & (dist <= EARLY)

    def stage(d, _):
        @pl.when(d >= 1)
        def _():
            for j in range(1, Y):
                forward(d, peer_y(j))

        def visit(i, _):
            side, k = i // X, lax.rem(i, X)
            dist = jnp.where(k == 0, d, d - 1)
            zb = jnp.where(side == 0, z - dist, z + dist)
            xb = lax.rem(x + k, X)
            ok = (zb >= 0) & (zb < Z) & (dist >= 0) & ((dist > 0) | (side == 0))

            @pl.when(ok)
            def _():
                @pl.when(k > 0)
                def _():
                    for u in range(Y * SUB):
                        kv_wait(zb, xb, u)

                attend(zb * X + xb, far_side)

                @pl.when(early(dist, xb))
                def _():
                    attend(zb * X + xb, near_side)

            return 0

        lax.fori_loop(0, 2 * X, visit, 0)
        forward(d + 3, y)
        return 0

    lax.fori_loop(0, Z + 1, stage, 0)
    settle(far_side, 0)

    def pair_copy(j, n):
        cols = pl.ds(n * NW, NW)
        return pltpu.make_async_remote_copy(
            src_ref=pb.at[j, 1 - c, :, cols], dst_ref=rb.at[j, :, cols],
            send_sem=ps_sem.at[j, n], recv_sem=pr_sem.at[j, n],
            device_id=(s_id, partner), device_id_type=MESH,
        )

    def far_copy(j, n):
        cols = pl.ds(n * NW, NW)
        return pltpu.make_async_remote_copy(
            src_ref=sb.at[j, :, cols], dst_ref=fb.at[j, :, cols],
            send_sem=ys_sem.at[j, n], recv_sem=yr_sem.at[j, n],
            device_id=(s_id, peer_y(j + 1) * CORES + c), device_id_type=MESH,
        )

    def pair_sum(j, n):
        cols = pl.ds(n * NW, NW)
        pair_copy(j, n).wait_recv()
        return pb[j, c, :, cols].astype(F32) + rb[j, :, cols].astype(F32)

    def project(i, _):
        @pl.when(i != (Y - 1) * NO)
        def _():
            ahead = jnp.where(i < (Y - 1) * NO, i, i - 1)
            j, n = ahead // NO, lax.rem(ahead, NO)
            cols = pl.ds(n * NW, NW)

            @pl.when(j == 0)
            def _():
                wo_copy(n).wait()

            part = jnp.dot(
                att[pl.ds(j * G, G), :], wo[:, cols], preferred_element_type=F32
            ).astype(BF16)
            for e in range(CORES):
                pb[j, e, :, cols] = part[e * r:(e + 1) * r, :]
            pair_copy(j, n).start()

        @pl.when((i > 0) & (i <= (Y - 1) * NO))
        def _():
            j, n = (i - 1) // NO, lax.rem(i - 1, NO)
            sb[j, :, pl.ds(n * NW, NW)] = pair_sum(j, n).astype(BF16)
            far_copy(j, n).start()

        return 0

    lax.fori_loop(0, (Y - 1) * NO + 1, project, 0)

    def rest_of(slot, _):
        zb, xb = slot // X, lax.rem(slot, X)
        dist = jnp.maximum(z - zb, zb - z)

        @pl.when(jnp.logical_not(early(dist, xb)))
        def _():
            attend(slot, near_side)

        return 0

    lax.fori_loop(0, Z * X, rest_of, 0)
    settle(near_side, (Y - 1) * G)
    lax.fori_loop((Y - 1) * NO + 1, Y * NO + 1, project, 0)

    def finish(n, _):
        total = pair_sum(Y - 1, n)
        for j in range(Y - 1):
            far_copy(j, n).wait_recv()
            total = total + fb[j, :, pl.ds(n * NW, NW)].astype(F32)
        out[:, pl.ds(n * NW, NW)] = total.astype(BF16)
        return 0

    lax.fori_loop(0, NO, finish, 0)

    def drain_hidden(k, _):
        hid_pair(k).wait_send()
        for j in range(1, Y):
            hid_send(j, k).wait_send()
            hid_relay(j, k).wait_send()
        return 0

    lax.fori_loop(0, NC, drain_hidden, 0)

    def drain_kv(zb, _):
        for u in range(Y * SUB):
            kv_out(zb, u, zb <= z, zb >= z, sent)
        return 0

    lax.fori_loop(0, Z, drain_kv, 0)

    def drain_out(n, _):
        for j in range(Y):
            pair_copy(j, n).wait_send()
        for j in range(Y - 1):
            far_copy(j, n).wait_send()
        return 0

    lax.fori_loop(0, NO, drain_out, 0)


def on_device(X, Z, Y, hidden, block_order, segment_ids, w_query, key_weight, value_weight, w_out):
    r, D = hidden.shape
    S, H = X * Z, Y * CORES
    R = r * H
    G = R // Y
    Cq, Ck = w_query.shape[1], key_weight.shape[1]
    W = Cq + 2 * Ck
    q_heads = Cq // HEAD_SIZE
    NC = NO = max(1, D // 512)
    exponent = np.arange(HEAD_SIZE // 2, dtype=np.float64) * 2.0 / HEAD_SIZE
    freqs = np.tile(ROPE_BASE ** (-exponent), 2).astype(np.float32)[None, :]
    dma = pltpu.SemaphoreType.DMA
    kv_heads = Ck // HEAD_SIZE
    group = q_heads // kv_heads

    def half_scratch(rows):
        together = 2 if rows % HEAD_SIZE == 0 and group % 2 == 0 else group
        lanes = group * rows
        return [
            pltpu.VMEM((kv_heads, lanes, HEAD_SIZE), BF16),
            pltpu.VMEM((kv_heads, lanes), F32),
            pltpu.VMEM((kv_heads, lanes), F32),
            pltpu.VMEM((kv_heads, HEAD_SIZE, lanes), F32),
            pltpu.VMEM((R, together * rows), F32),
            pltpu.VMEM((2, together * rows), jnp.int32),
        ]

    far = max(1, Y - 1)
    vmem = pl.BlockSpec(memory_space=pltpu.VMEM)
    anywhere = pl.BlockSpec(memory_space=pl.ANY)
    return pl.pallas_call(
        functools.partial(kernel, X, Z, Y, NC, NO),
        out_shape=jax.ShapeDtypeStruct((r, D), BF16),
        in_specs=[pl.BlockSpec(memory_space=pltpu.SMEM), vmem, vmem, vmem] + [anywhere] * 4,
        out_specs=vmem,
        scratch_shapes=[
            pltpu.VMEM((R, D), BF16),
            pltpu.VMEM((D, W), BF16),
            pltpu.VMEM((Cq, D), BF16),
            pltpu.VMEM((G, W), F32),
            pltpu.VMEM((R, HEAD_SIZE), F32),
            pltpu.VMEM((R, HEAD_SIZE), F32),
            pltpu.VMEM((S, R, 2 * Ck), BF16),
            pltpu.VMEM((R, Cq), BF16),
            pltpu.VMEM((Y, CORES, r, D), BF16),
            pltpu.VMEM((Y, r, D), BF16),
            pltpu.VMEM((far, r, D), BF16),
            pltpu.VMEM((far, r, D), BF16),
            *half_scratch((Y - 1) * G),
            *half_scratch(G),
            dma((3, NC)), dma((NO,)),
            dma((Y, NC)), dma((NC,)), dma((Y, NC)), dma((H, NC)),
            dma((Z, Y * SUB, 1 + X)), dma((S, Y * SUB)),
            dma((Y, NO)), dma((Y, NO)), dma((far, NO)), dma((far, NO)),
        ],
        compiler_params=pltpu.CompilerParams(
            collective_id=0, has_side_effects=True, vmem_limit_bytes=60 * 1024 * 1024
        ),
    )(
        block_order, hidden, segment_ids.reshape(block_order.shape[0], -1), jnp.asarray(freqs),
        w_query, key_weight, value_weight, w_out,
    )


def solution(mesh):
    seq, head = mesh.shape["seq"], mesh.shape["head"]
    X = 1
    while 4 * X * X <= seq and seq % (2 * X) == 0:
        X *= 2
    placed = (
        P(("seq", "head"), None),
        P(),
        P(),
        P(None, "head"),
        P(None, "head"),
        P(None, "head"),
        P("head", None),
    )
    return jax.shard_map(
        functools.partial(on_device, X, seq // X, head // CORES),
        mesh=mesh, in_specs=placed, out_specs=P(("seq", "head"), None), check_vma=False,
    )
```

```python
import functools
import math

import jax
import jax.numpy as jnp
import numpy as np
from jax import lax
from jax.experimental import pallas as pl
from jax.experimental.pallas import tpu as pltpu
from jax.sharding import PartitionSpec as P

HEAD_SIZE = 128
NEGATIVE_FILLER = -1e30
ROPE_BASE = 500000.0
DOCS = 4
CORES = 2
SUB = 2
EARLY = 2
MESH = pl.DeviceIdType.MESH
F32 = jnp.float32
BF16 = jnp.bfloat16


def rotated(t, cosine, sine):
    heads = t.shape[1] // HEAD_SIZE
    pieces = []
    for h in range(heads):
        one = t[:, h * HEAD_SIZE:(h + 1) * HEAD_SIZE]
        pieces.append(one * cosine + pltpu.roll(one, HEAD_SIZE // 2, 1) * sine)
    return pieces


def kernel(
    X, Z, Y, NC, NO,
    order, hidden, seg, freq, wq, wk, wv, wo_hbm, out,
    xg, wb, wo, acc, cos_t, sin_t, kv, att, pb, rb, sb, fb, *rest,
):
    far_side, near_side = rest[:6], rest[6:12]
    (w_sem, wo_sem, hs_sem, hp_sem, hl_sem, hr_sem,
     ks_sem, kr_sem, ps_sem, pr_sem, ys_sem, yr_sem) = rest[12:]
    r, D = hidden.shape
    R = xg.shape[0]
    G = R // Y
    Cq, Ck = wq.shape[1], wk.shape[1]
    half = R // 2
    q_heads, kv_heads = Cq // HEAD_SIZE, Ck // HEAD_SIZE
    group = q_heads // kv_heads
    KW, NW = D // NC, D // NO
    s_id, h_id = lax.axis_index("seq"), lax.axis_index("head")
    y, c = h_id // CORES, h_id % CORES
    z, x = s_id // X, s_id % X
    partner = y * CORES + (1 - c)

    def peer_y(j):
        return lax.rem(y + j, Y)

    def w_copy(which, k):
        src = (wq, wk, wv)[which]
        col = (0, Cq, Cq + Ck)[which]
        rows = pl.ds(k * KW, KW)
        return pltpu.make_async_copy(
            src.at[rows, :], wb.at[rows, pl.ds(col, src.shape[1])], w_sem.at[which, k]
        )

    def wo_copy(n):
        cols = pl.ds(n * NW, NW)
        return pltpu.make_async_copy(wo_hbm.at[:, cols], wo.at[:, cols], wo_sem.at[n])

    for k in range(NC):
        w_copy(1, k).start()
        w_copy(2, k).start()

    barrier = pltpu.get_barrier_semaphore()

    def greet(sq, hd):
        pl.semaphore_signal(barrier, inc=1, device_id=(sq, hd), device_id_type=MESH)

    greet(s_id, partner)
    for j in range(1, Y):
        greet(s_id, peer_y(j) * CORES + c)
    for k in range(1, X):
        greet(z * X + lax.rem(x + k, X), h_id)

    @pl.when(z > 0)
    def _():
        greet(s_id - X, h_id)

    @pl.when(z < Z - 1)
    def _():
        greet(s_id + X, h_id)

    near = jnp.where(z > 0, 1, 0) + jnp.where(z < Z - 1, 1, 0)
    pl.semaphore_wait(barrier, 1 + (Y - 1) + (X - 1) + near)

    def hid_copy(origin, k, target, sem, from_input):
        cols = pl.ds(k * KW, KW)
        rows = pl.ds(origin * r, r)
        src = hidden.at[:, cols] if from_input else xg.at[rows, cols]
        return pltpu.make_async_remote_copy(
            src_ref=src, dst_ref=xg.at[rows, cols], send_sem=sem, recv_sem=hr_sem.at[origin, k],
            device_id=(s_id, target), device_id_type=MESH,
        )

    def hid_send(j, k):
        return hid_copy(h_id, k, peer_y(j) * CORES + c, hs_sem.at[j, k], True)

    def hid_pair(k):
        return hid_copy(h_id, k, partner, hp_sem.at[k], True)

    def hid_relay(j, k):
        return hid_copy(peer_y(j) * CORES + c, k, partner, hl_sem.at[j, k], False)

    def hid_from(origin, k):
        return hid_copy(origin, k, partner, hp_sem.at[k], False)

    for k in range(NC):
        hid_pair(k).start()
        for j in range(1, Y):
            hid_send(j, k).start()

    xg[pl.ds(h_id * r, r), :] = hidden[...]

    lane = lax.broadcasted_iota(jnp.int32, (half, HEAD_SIZE), 1)
    row = lax.broadcasted_iota(jnp.int32, (half, HEAD_SIZE), 0)
    for i in range(2):
        base = order[2 * s_id + i]
        angle = (row + base * half).astype(F32) * freq[...]
        cos_t[pl.ds(i * half, half), :] = jnp.cos(angle)
        sn = jnp.sin(angle)
        sin_t[pl.ds(i * half, half), :] = jnp.where(lane < HEAD_SIZE // 2, -sn, sn)

    starts = [
        jnp.sum(jnp.sum((seg[...] < v).astype(jnp.int32), axis=0, keepdims=True), axis=1, keepdims=True)
        for v in range(1, DOCS)
    ]
    for side, places in ((far_side, range(1, Y)), (near_side, (0,))):
        info = side[5]
        for i, j in enumerate(places):
            first = peer_y(j) * G
            pos = lax.broadcasted_iota(jnp.int32, (1, G), 1) + (
                order[2 * s_id + first // half] * half + lax.rem(first, half)
            )
            start = jnp.zeros_like(pos)
            for begun in starts:
                start = jnp.where(begun <= pos, jnp.maximum(start, begun), start)
            wide = len(places) * G
            for gh in range(info.shape[1] // wide):
                lanes = slice(gh * wide + i * G, gh * wide + (i + 1) * G)
                info[0:1, lanes] = pos
                info[1:2, lanes] = start

    B = G // SUB

    def kv_copy(zb, xb, u, target, way):
        slot = zb * X + xb
        rows = pl.ds(u * B, B)
        return pltpu.make_async_remote_copy(
            src_ref=kv.at[slot, rows, :], dst_ref=kv.at[slot, rows, :],
            send_sem=ks_sem.at[zb, u, way], recv_sem=kr_sem.at[slot, u],
            device_id=(target, h_id), device_id_type=MESH,
        )

    def kv_out(zb, u, up, down, act):
        @pl.when(up & (z < Z - 1))
        def _():
            act(kv_copy(zb, x, u, s_id + X, 0))

        @pl.when(down & (z > 0))
        def _():
            act(kv_copy(zb, x, u, s_id - X, 1))

        for k in range(1, X):
            act(kv_copy(zb, x, u, z * X + lax.rem(x + k, X), 1 + k))

    def kv_wait(zb, xb, u):
        kv_copy(zb, xb, u, s_id, 0).wait_recv()

    start_it = lambda cp: cp.start()
    sent = lambda cp: cp.wait_send()

    def forward(d, g):
        for e in range(SUB):
            u = g * SUB + e

            @pl.when((d < Z) & (z - d >= 0))
            def _():
                kv_wait(z - d, x, u)
                kv_out(z - d, u, True, False, start_it)

            @pl.when((d < Z) & (z + d < Z))
            def _():
                kv_wait(z + d, x, u)
                kv_out(z + d, u, False, True, start_it)

    def store_kv(g):
        rows = pl.ds(g * G, G)
        pieces = rotated(acc[:, Cq:Cq + Ck], cos_t[rows, :], sin_t[rows, :])
        for h in range(kv_heads):
            kv[s_id, rows, h * HEAD_SIZE:(h + 1) * HEAD_SIZE] = pieces[h].astype(BF16)
        kv[s_id, rows, Ck:2 * Ck] = acc[:, Cq + Ck:].astype(BF16)
        for e in range(SUB):
            kv_out(z, g * SUB + e, True, True, start_it)

    def store_q(g, side, place):
        rows = pl.ds(g * G, G)
        q = side[0]
        wide = q.shape[1] // group
        pieces = rotated(acc[:, :Cq], cos_t[rows, :], sin_t[rows, :])
        for h in range(q_heads):
            lo = (h % group) * wide + place * G
            q[h // group, lo:lo + G, :] = pieces[h].astype(BF16)

    def add_dot(g, k, lo, hi):
        span = pl.ds(k * KW, KW)
        acc[:, lo:hi] += jnp.dot(
            xg[pl.ds(g * G, G), span], wb[span, lo:hi], preferred_element_type=F32
        )

    acc[...] = jnp.zeros_like(acc)

    def first_kv(k, _):
        hid_from(partner, k).wait_recv()
        w_copy(1, k).wait()
        w_copy(2, k).wait()
        w_copy(0, k).start()
        add_dot(y, k, Cq, Cq + 2 * Ck)
        return 0

    lax.fori_loop(0, NC, first_kv, 0)
    store_kv(y)

    def first_q(k, _):
        w_copy(0, k).wait()
        wo_copy(k).start()
        add_dot(y, k, 0, Cq)
        return 0

    lax.fori_loop(0, NC, first_q, 0)
    store_q(y, near_side, 0)

    for j in range(1, Y):
        g = peer_y(j)
        acc[...] = jnp.zeros_like(acc)

        def arrive(k, _, j=j, g=g):
            @pl.when(k < NC)
            def _():
                hid_from(g * CORES + c, k).wait_recv()
                hid_relay(j, k).start()

            @pl.when(k > 0)
            def _():
                hid_from(g * CORES + (1 - c), k - 1).wait_recv()
                add_dot(g, k - 1, 0, Cq + 2 * Ck)

            if j == 1:
                @pl.when(k == NC // 2)
                def _():
                    forward(1, y)

                @pl.when(k == NC)
                def _():
                    forward(2, y)

            return 0

        lax.fori_loop(0, NC + 1, arrive, 0)
        store_kv(g)
        store_q(g, far_side, j - 1)

    for side in (far_side, near_side):
        side[1][...] = jnp.full_like(side[1], NEGATIVE_FILLER)
        side[2][...] = jnp.zeros_like(side[2])
        side[3][...] = jnp.zeros_like(side[3])
    scale = math.log2(math.e) / math.sqrt(HEAD_SIZE)
    nt = (((1,), (1,)), ((), ()))

    def attend(slot, side):
        q, m_s, l_s, o_s, bias, info = side
        chunk = bias.shape[1]
        krow = lax.broadcasted_iota(jnp.int32, (half, chunk), 0)
        for i in range(2):
            kpos = krow + order[2 * slot + i] * half
            ok = (kpos <= info[0:1, :]) & (kpos >= info[1:2, :])
            bias[i * half:(i + 1) * half, :] = jnp.where(ok, 0.0, NEGATIVE_FILLER)
        work = [(kh, w) for kh in range(kv_heads) for w in range(q.shape[1] // chunk)]
        span = lambda w: slice(w * chunk, (w + 1) * chunk)
        keys = [kv[slot, :, kh * HEAD_SIZE:(kh + 1) * HEAD_SIZE] for kh in range(kv_heads)]
        vals = [
            kv[slot, :, Ck + kh * HEAD_SIZE:Ck + (kh + 1) * HEAD_SIZE].T for kh in range(kv_heads)
        ]

        def scores(item):
            kh, w = item
            return lax.dot_general(keys[kh], q[kh, span(w), :], nt, preferred_element_type=F32)

        ahead = scores(work[0])
        for i, (kh, w) in enumerate(work):
            raw = ahead
            if i + 1 < len(work):
                ahead = scores(work[i + 1])
            cols = span(w)
            s = raw * scale + bias[...]
            old = m_s[kh:kh + 1, cols]
            new = jnp.maximum(old, jnp.max(s, axis=0, keepdims=True))
            p = jnp.exp2(s - new)
            alpha = jnp.exp2(old - new)
            m_s[kh:kh + 1, cols] = new
            l_s[kh:kh + 1, cols] = l_s[kh:kh + 1, cols] * alpha + jnp.sum(p, axis=0, keepdims=True)
            o_s[kh, :, cols] = o_s[kh, :, cols] * alpha + jnp.dot(
                vals[kh], p.astype(BF16), preferred_element_type=F32
            )

    def settle(side, lo):
        q, m_s, l_s, o_s, bias, info = side
        wide = q.shape[1] // group
        for h in range(q_heads):
            kh, gh = h // group, h % group
            lanes = slice(gh * wide, (gh + 1) * wide)
            att[lo:lo + wide, h * HEAD_SIZE:(h + 1) * HEAD_SIZE] = (
                o_s[kh, :, lanes] / l_s[kh:kh + 1, lanes]
            ).T.astype(BF16)

    def early(dist, xb):
        return (xb == x) & (dist <= EARLY)

    def stage(d, _):
        @pl.when(d >= 1)
        def _():
            for j in range(1, Y):
                forward(d, peer_y(j))

        def visit(i, _):
            side, k = i // X, lax.rem(i, X)
            dist = jnp.where(k == 0, d, d - 1)
            zb = jnp.where(side == 0, z - dist, z + dist)
            xb = lax.rem(x + k, X)
            ok = (zb >= 0) & (zb < Z) & (dist >= 0) & ((dist > 0) | (side == 0))

            @pl.when(ok)
            def _():
                @pl.when(k > 0)
                def _():
                    for u in range(Y * SUB):
                        kv_wait(zb, xb, u)

                attend(zb * X + xb, far_side)

                @pl.when(early(dist, xb))
                def _():
                    attend(zb * X + xb, near_side)

            return 0

        lax.fori_loop(0, 2 * X, visit, 0)
        forward(d + 3, y)
        return 0

    lax.fori_loop(0, Z + 1, stage, 0)
    settle(far_side, 0)

    def pair_copy(j, n):
        cols = pl.ds(n * NW, NW)
        return pltpu.make_async_remote_copy(
            src_ref=pb.at[j, 1 - c, :, cols], dst_ref=rb.at[j, :, cols],
            send_sem=ps_sem.at[j, n], recv_sem=pr_sem.at[j, n],
            device_id=(s_id, partner), device_id_type=MESH,
        )

    def far_copy(j, n):
        cols = pl.ds(n * NW, NW)
        return pltpu.make_async_remote_copy(
            src_ref=sb.at[j, :, cols], dst_ref=fb.at[j, :, cols],
            send_sem=ys_sem.at[j, n], recv_sem=yr_sem.at[j, n],
            device_id=(s_id, peer_y(j + 1) * CORES + c), device_id_type=MESH,
        )

    def pair_sum(j, n):
        cols = pl.ds(n * NW, NW)
        pair_copy(j, n).wait_recv()
        return pb[j, c, :, cols].astype(F32) + rb[j, :, cols].astype(F32)

    def project(i, _):
        @pl.when(i != (Y - 1) * NO)
        def _():
            ahead = jnp.where(i < (Y - 1) * NO, i, i - 1)
            j, n = ahead // NO, lax.rem(ahead, NO)
            cols = pl.ds(n * NW, NW)

            @pl.when(j == 0)
            def _():
                wo_copy(n).wait()

            part = jnp.dot(
                att[pl.ds(j * G, G), :], wo[:, cols], preferred_element_type=F32
            ).astype(BF16)
            for e in range(CORES):
                pb[j, e, :, cols] = part[e * r:(e + 1) * r, :]
            pair_copy(j, n).start()

        @pl.when((i > 0) & (i <= (Y - 1) * NO))
        def _():
            j, n = (i - 1) // NO, lax.rem(i - 1, NO)
            sb[j, :, pl.ds(n * NW, NW)] = pair_sum(j, n).astype(BF16)
            far_copy(j, n).start()

        return 0

    lax.fori_loop(0, (Y - 1) * NO + 1, project, 0)

    def rest_of(slot, _):
        zb, xb = slot // X, lax.rem(slot, X)
        dist = jnp.maximum(z - zb, zb - z)

        @pl.when(jnp.logical_not(early(dist, xb)))
        def _():
            attend(slot, near_side)

        return 0

    lax.fori_loop(0, Z * X, rest_of, 0)
    settle(near_side, (Y - 1) * G)
    lax.fori_loop((Y - 1) * NO + 1, Y * NO + 1, project, 0)

    def finish(n, _):
        total = pair_sum(Y - 1, n)
        for j in range(Y - 1):
            far_copy(j, n).wait_recv()
            total = total + fb[j, :, pl.ds(n * NW, NW)].astype(F32)
        out[:, pl.ds(n * NW, NW)] = total.astype(BF16)
        return 0

    lax.fori_loop(0, NO, finish, 0)

    def drain_hidden(k, _):
        hid_pair(k).wait_send()
        for j in range(1, Y):
            hid_send(j, k).wait_send()
            hid_relay(j, k).wait_send()
        return 0

    lax.fori_loop(0, NC, drain_hidden, 0)

    def drain_kv(zb, _):
        for u in range(Y * SUB):
            kv_out(zb, u, zb <= z, zb >= z, sent)
        return 0

    lax.fori_loop(0, Z, drain_kv, 0)

    def drain_out(n, _):
        for j in range(Y):
            pair_copy(j, n).wait_send()
        for j in range(Y - 1):
            far_copy(j, n).wait_send()
        return 0

    lax.fori_loop(0, NO, drain_out, 0)


def on_device(X, Z, Y, hidden, block_order, segment_ids, w_query, key_weight, value_weight, w_out):
    r, D = hidden.shape
    S, H = X * Z, Y * CORES
    R = r * H
    G = R // Y
    Cq, Ck = w_query.shape[1], key_weight.shape[1]
    W = Cq + 2 * Ck
    q_heads = Cq // HEAD_SIZE
    NC = NO = max(1, D // 512)
    exponent = np.arange(HEAD_SIZE // 2, dtype=np.float64) * 2.0 / HEAD_SIZE
    freqs = np.tile(ROPE_BASE ** (-exponent), 2).astype(np.float32)[None, :]
    dma = pltpu.SemaphoreType.DMA
    kv_heads = Ck // HEAD_SIZE
    group = q_heads // kv_heads

    def half_scratch(rows):
        together = 2 if rows % HEAD_SIZE == 0 and group % 2 == 0 else group
        lanes = group * rows
        return [
            pltpu.VMEM((kv_heads, lanes, HEAD_SIZE), BF16),
            pltpu.VMEM((kv_heads, lanes), F32),
            pltpu.VMEM((kv_heads, lanes), F32),
            pltpu.VMEM((kv_heads, HEAD_SIZE, lanes), F32),
            pltpu.VMEM((R, together * rows), F32),
            pltpu.VMEM((2, together * rows), jnp.int32),
        ]

    far = max(1, Y - 1)
    vmem = pl.BlockSpec(memory_space=pltpu.VMEM)
    anywhere = pl.BlockSpec(memory_space=pl.ANY)
    return pl.pallas_call(
        functools.partial(kernel, X, Z, Y, NC, NO),
        out_shape=jax.ShapeDtypeStruct((r, D), BF16),
        in_specs=[pl.BlockSpec(memory_space=pltpu.SMEM), vmem, vmem, vmem] + [anywhere] * 4,
        out_specs=vmem,
        scratch_shapes=[
            pltpu.VMEM((R, D), BF16),
            pltpu.VMEM((D, W), BF16),
            pltpu.VMEM((Cq, D), BF16),
            pltpu.VMEM((G, W), F32),
            pltpu.VMEM((R, HEAD_SIZE), F32),
            pltpu.VMEM((R, HEAD_SIZE), F32),
            pltpu.VMEM((S, R, 2 * Ck), BF16),
            pltpu.VMEM((R, Cq), BF16),
            pltpu.VMEM((Y, CORES, r, D), BF16),
            pltpu.VMEM((Y, r, D), BF16),
            pltpu.VMEM((far, r, D), BF16),
            pltpu.VMEM((far, r, D), BF16),
            *half_scratch((Y - 1) * G),
            *half_scratch(G),
            dma((3, NC)), dma((NO,)),
            dma((Y, NC)), dma((NC,)), dma((Y, NC)), dma((H, NC)),
            dma((Z, Y * SUB, 1 + X)), dma((S, Y * SUB)),
            dma((Y, NO)), dma((Y, NO)), dma((far, NO)), dma((far, NO)),
        ],
        compiler_params=pltpu.CompilerParams(
            collective_id=0, has_side_effects=True, vmem_limit_bytes=60 * 1024 * 1024
        ),
    )(
        block_order, hidden, segment_ids.reshape(block_order.shape[0], -1), jnp.asarray(freqs),
        w_query, key_weight, value_weight, w_out,
    )


def solution(mesh):
    seq, head = mesh.shape["seq"], mesh.shape["head"]
    X = 1
    while 4 * X * X <= seq and seq % (2 * X) == 0:
        X *= 2
    placed = (
        P(("seq", "head"), None),
        P(),
        P(),
        P(None, "head"),
        P(None, "head"),
        P(None, "head"),
        P("head", None),
    )
    return jax.shard_map(
        functools.partial(on_device, X, seq // X, head // CORES),
        mesh=mesh, in_specs=placed, out_specs=P(("seq", "head"), None), check_vma=False,
    )
```
